128 devices in a mesh: batch: 32 (over z, y, x_hi), mp: 4 (over x_lo, core).
Axes of the slice: x: 4 (x_hi: 2, x_lo: 2; x = x_hi * 2 + x_lo), y: 4, z: 4, core: 2. Of those that a mesh axis runs over, the one named last changes fastest.
Arguments:
- lookup_ids: int32 [64, 65536], P('batch'), may hold values from 0 to 8191
- table_feature: int32 [64], replicated, may hold values from 0 to 63, each once
- tables: bfloat16 [64, 8192, 128], P('batch'), may hold values from -6 to 6
- cross_down: bfloat16 [2, 8192, 512], P(None, 'mp'), may hold values from -0.0625 to 0.0625
- cross_up: bfloat16 [2, 512, 8192], P(None, None, 'mp'), may hold values from -0.25 to 0.25
- cross_bias: float32 [2, 8192], P(None, 'mp'), may hold values from -3 to 3
Outputs:
- crossed: bfloat16 [65536, 8192], P('batch', 'mp')
The draws below stay inside these ranges and needn't reach their ends.
Inputs may be any that keep to these rules, and one draw needn't show every extreme that they name: `table_feature`: each number appears once.
All inputs are finite; a program needn't handle non-finite values.
Results may differ from the reference program's by a relative error of at most 0.015.
Values may be sent and summed in bfloat16 or wider, within the bound.
A program may use at most 128 MiB of HBM per device.

```python
import math
import jax
import jax.numpy as jnp
import numpy as np
from jax import lax

FEATS = 64
EMB = 128
RANK = 512
ROWS = 8192
LAYERS = 2
WIDTH = 8192
BATCH = 65536
N_MP = 4


def plant(drawn, stream_key, low, top_value):
    place = [jax.random.randint(jax.random.fold_in(stream_key, axis), (), 0, length) for axis, length in enumerate(drawn.shape)]
    main_axis = drawn.shape.index(max(drawn.shape))
    neighbour = place[:main_axis] + [(place[main_axis] + 1) % drawn.shape[main_axis]] + place[main_axis + 1:]
    return drawn.at[tuple(place)].set(low).at[tuple(neighbour)].set(top_value)


def shard_levels(own_key, dims, pieces, low, high):
    factor_of = 1.0
    for axis_at, blocks in pieces:
        draws = jax.random.uniform(jax.random.fold_in(jax.random.fold_in(own_key, 6), axis_at), (blocks,), jnp.float32, low / len(pieces), high / len(pieces))
        factor_of = factor_of * jnp.repeat(jnp.exp(draws), dims[axis_at] // blocks).reshape((-1,) + (1,) * (len(dims) - 1 - axis_at))
    return factor_of


def rank_table(number_of, slope):
    weights = [(1 << 20) // math.isqrt(rank ** slope) + 1 for rank in range(1, number_of + 1)]
    width = 1 + sum(weights) // (1 << 30)
    return np.cumsum(np.array([max(1, weight // width) for weight in weights]))


def skewed_ids(stream_key, shape, amount, slope):
    grid = rank_table(amount, slope)
    lot = jax.random.randint(jax.random.fold_in(stream_key, 1), shape, 0, int(grid[amount - 1]))
    standing = jnp.searchsorted(jnp.asarray(grid, jnp.int32), lot, side="right")
    return jax.random.permutation(jax.random.fold_in(stream_key, 2), amount)[standing].astype(jnp.int32)


def centred(key, extent, width, bound, cuts=(), held_as=jnp.bfloat16):
    values = jax.random.normal(key, extent, jnp.float32) * width
    if len(cuts) > 0:
        values = shard_levels(key, extent, cuts, -0.22, 0.18) * values
    return jnp.clip(values, min=-bound, max=bound).astype(held_as)


def setup_inputs(seed: int = 0) -> dict:
    streams_of = jax.random.split(jax.random.key(seed), 7)
    lookup_ids = plant(skewed_ids(streams_of[0], (FEATS, BATCH), ROWS, 2), jax.random.fold_in(streams_of[0], 3), 0, ROWS - 1).astype(jnp.int32)
    table_feature = jax.random.permutation(streams_of[1], FEATS).astype(jnp.int32)
    tables = centred(streams_of[2], (FEATS, ROWS, EMB), 1.0, 6.0, ((0, 32),))
    cross_down = centred(streams_of[3], (LAYERS, WIDTH, RANK), WIDTH ** -0.5, 0.0625, ((1, 4),))
    cross_up = centred(streams_of[4], (LAYERS, RANK, WIDTH), RANK ** -0.5, 0.25, ((2, 4),))
    cross_bias = centred(streams_of[5], (LAYERS, WIDTH), 0.5, 3.0, ((1, 4),), jnp.float32)
    return dict(lookup_ids=lookup_ids, table_feature=table_feature, tables=tables, cross_down=cross_down, cross_up=cross_up, cross_bias=cross_bias)


def reference(lookup_ids, table_feature, tables, cross_down, cross_up, cross_bias):
    looked = jax.vmap(lambda table, index: jnp.take(table, index, axis=0))(tables, lookup_ids)
    inverse = jnp.zeros((FEATS,), jnp.int32).at[table_feature].set(jnp.arange(FEATS, dtype=jnp.int32))
    by_feature = jnp.take(looked, inverse, axis=0)
    embedded = jnp.transpose(by_feature, (1, 2, 0)).reshape(BATCH, EMB * FEATS)
    block = WIDTH // N_MP
    state = embedded
    for layer in range(LAYERS):
        low_sum = jnp.zeros((BATCH, RANK), jnp.float32)
        for piece in range(N_MP):
            term = jnp.dot(state[:, piece * block:(piece + 1) * block], cross_down[layer, piece * block:(piece + 1) * block, :], preferred_element_type=jnp.float32)
            rounded = lax.optimization_barrier(term.astype(jnp.bfloat16))
            low_sum = low_sum + rounded.astype(jnp.float32)
        low = low_sum.astype(jnp.bfloat16)
        high = jnp.dot(low, cross_up[layer], preferred_element_type=jnp.float32) + cross_bias[layer][None, :]
        state = (embedded.astype(jnp.float32) * high + state.astype(jnp.float32)).astype(jnp.bfloat16)
    return state
```

```python
import functools

import jax
import jax.numpy as jnp
from jax import lax
from jax.experimental import pallas as pl
from jax.experimental.pallas import tpu as pltpu
from jax.sharding import PartitionSpec as P

MESH = pl.DeviceIdType.MESH
UNROLL = 64
F32 = jnp.float32
BF16 = jnp.bfloat16


def kernel(
    sizes,
    ids,
    tables,
    placing,
    downs,
    ups,
    bias,
    out,
    table,
    rows,
    pick,
    message,
    landed,
    emb,
    state,
    weight_down,
    weight_up,
    part,
    near,
    summed,
    far,
    low,
    send_sem,
    recv_sem,
    load_sem,
    out_sem,
    hop_send,
    hop_recv,
):
    groups, members, chunks, share, slot_rows = sizes
    peers = groups * members
    b = lax.axis_index("batch")
    m = lax.axis_index("mp")
    me = b * members + m
    core = lax.rem(m, 2)
    partner = {"mp": m + 1 - 2 * core}
    across = {"mp": lax.rem(m + 2, 4)}
    width = emb.shape[2]
    rank = low.shape[2]
    tile = members * share
    half = tile // 2
    mine = pl.multiple_of(core * half, half)
    theirs = pl.multiple_of((1 - core) * half, half)

    barrier = pltpu.get_barrier_semaphore()

    def greet(i, _):
        other = lax.rem(me + i, peers)
        pl.semaphore_signal(
            barrier,
            inc=1,
            device_id={"batch": other // members, "mp": lax.rem(other, members)},
            device_id_type=MESH,
        )
        return 0

    held = tables.shape[0]
    first = chunks - held
    load_table = pltpu.make_async_copy(tables, message.at[pl.ds(first, held)], load_sem.at[0])
    load_table.start()
    load_down = pltpu.make_async_copy(downs, weight_down, load_sem.at[1])
    load_down.start()
    load_up = pltpu.make_async_copy(ups, weight_up, load_sem.at[2])
    load_up.start()
    lax.fori_loop(1, peers, greet, 0)

    row = lax.broadcasted_iota(jnp.int32, (256, 256), 0)
    col = lax.broadcasted_iota(jnp.int32, (256, 256), 1)
    wanted = ((row // 4) % 2) * 128 + (row // 8) * 4 + row % 4
    pick[...] = (wanted == col).astype(BF16)

    load_table.wait()

    block_rows = message.shape[2]
    for slot in range(held):

        def widen(i, _):
            at = pl.multiple_of(slot * slot_rows + i * block_rows, block_rows)
            table[pl.ds(at, block_rows), :] = message[first + slot, i].astype(F32)
            return 0

        lax.fori_loop(0, slot_rows // block_rows, widen, 0)

    def look(chunk, dest):
        def group(g, _):
            for u in range(UNROLL):
                for slot in range(2):
                    index = ids[(dest * chunks + chunk) * (2 * share) + slot * share + g * UNROLL + u]
                    rows[g, u : u + 1, slot * 128 : (slot + 1) * 128] = table[
                        pl.ds(index + slot * slot_rows, 1), :
                    ]
            return 0

        lax.fori_loop(0, share // UNROLL, group, 0)
        looked = rows[...].reshape(share, 256).astype(BF16)
        return (
            lax.dot_general(
                pick[...], looked, (((1,), (1,)), ((), ())), preferred_element_type=F32
            )
            .astype(BF16)
            .reshape(members, 64, share)
        )

    def send(chunk, dest, member):
        pltpu.make_async_remote_copy(
            src_ref=message.at[chunk, dest * members + member],
            dst_ref=landed.at[chunk, me],
            send_sem=send_sem.at[chunk],
            recv_sem=recv_sem.at[chunk],
            device_id={"batch": dest, "mp": member},
            device_id_type=MESH,
        ).start()

    def chunk_out(chunk, _):
        def one(i, _):
            dest = lax.rem(b + i, groups)
            message[chunk, pl.ds(dest * members, members)] = look(chunk, dest)

            @pl.when(jnp.logical_and(chunk == 0, i == 1))
            def _():
                pl.semaphore_wait(barrier, peers - 1)

            for k in range(members):
                send(chunk, dest, lax.rem(m + k, members))
            return 0

        lax.fori_loop(1, groups, one, 0)
        message[chunk, pl.ds(b * members, members)] = look(chunk, b)
        landed[chunk, me] = message[chunk, me]
        for k in range(1, members):
            send(chunk, b, lax.rem(m + k, members))
        return 0

    lax.fori_loop(0, chunks, chunk_out, 0)
    load_down.wait()
    load_up.wait()

    def hop(kind, t, src, dst, device):
        return pltpu.make_async_remote_copy(
            src_ref=src,
            dst_ref=dst,
            send_sem=hop_send.at[kind, t],
            recv_sem=hop_recv.at[kind, t],
            device_id=device,
            device_id_type=MESH,
        )

    def hop_near(layer, t):
        return hop(3 * layer, t, part.at[t, 1], near.at[t], partner)

    def hop_far(layer, t):
        return hop(3 * layer + 1, t, summed.at[t], far.at[layer, t], across)

    def hop_low(layer, t):
        there = low.at[t, pl.ds(mine, half)]
        return hop(3 * layer + 2, t, there, there, partner)

    def project(layer, t, source):
        for which, at in ((1, theirs), (0, mine)):
            product = jnp.dot(
                source[t, pl.ds(at, half), :], weight_down[layer], preferred_element_type=F32
            )
            part[t, which] = product.astype(BF16)
            if which == 1:
                hop_near(layer, t).start()

    def add_near(layer, t):
        hop_near(layer, t).wait()
        summed[t] = (part[t, 0].astype(F32) + near[t].astype(F32)).astype(BF16)
        hop_far(layer, t).start()

    def add_far(layer, t):
        hop_far(layer, t).wait()
        low[t, pl.ds(mine, half), :] = (
            summed[t].astype(F32) + far[layer, t].astype(F32)
        ).astype(BF16)
        hop_low(layer, t).start()

    def expand(layer, t, before):
        hop_low(layer, t).wait()

        def block(i, _):
            at = pl.ds(pl.multiple_of(i * 128, 128), 128)
            high = (
                jnp.dot(
                    low[t, at, :], weight_up[layer], preferred_element_type=F32
                )
                + bias[layer : layer + 1, :]
            )
            state[t, at, :] = (
                emb[t, at, :].astype(F32) * high + before[t, at, :].astype(F32)
            ).astype(BF16)
            return 0

        lax.fori_loop(0, tile // 128, block, 0)

    def place(t):
        pltpu.make_async_copy(
            message.at[t, pl.ds(0, peers - 1)], landed.at[t, pl.ds(0, peers - 1)], recv_sem.at[t]
        ).wait()

        def landed_of(t, i, hi):
            return jnp.concatenate(
                [landed[t, g * members + i, hi * 8 : (hi + 1) * 8, :] for g in range(groups)], axis=0
            )

        def member_rows(i, _):
            for hi in range(8):
                block = lax.dot_general(
                    landed_of(t, i, hi), placing[...], (((0,), (0,)), ((), ())), preferred_element_type=F32
                )
                emb[t, pl.ds(pl.multiple_of(i * share, share), share), hi * 256 : (hi + 1) * 256] = (
                    block.astype(BF16)
                )
            return 0

        lax.fori_loop(0, members, member_rows, 0)

    def store(t):
        return pltpu.make_async_copy(
            state.at[t], out.at[pl.ds(pl.multiple_of(t * tile, tile), tile)], out_sem.at[t]
        )

    def step(i, _):
        @pl.when(i >= 2)
        def _():
            expand(1, i - 2, state)
            store(i - 2).start()

        @pl.when(jnp.logical_and(i >= 1, i <= chunks))
        def _():
            expand(0, i - 1, emb)
            project(1, i - 1, state)

        @pl.when(i < chunks)
        def _():
            place(i)
            project(0, i, emb)

        @pl.when(jnp.logical_and(i >= 1, i <= chunks))
        def _():
            add_near(1, i - 1)

        @pl.when(i < chunks)
        def _():
            add_near(0, i)

        @pl.when(jnp.logical_and(i >= 1, i <= chunks))
        def _():
            add_far(1, i - 1)

        @pl.when(i < chunks)
        def _():
            add_far(0, i)

        return 0

    lax.fori_loop(0, chunks + 2, step, 0)

    def finish(t, _):
        store(t).wait()
        pltpu.make_async_copy(
            message.at[t, pl.ds(0, peers - 1)], landed.at[t, pl.ds(0, peers - 1)], send_sem.at[t]
        ).wait()
        return 0

    lax.fori_loop(0, chunks, finish, 0)


def per_device(lookup_ids, table_feature, tables, cross_down, cross_up, cross_bias):
    slots_local, slot_rows, emb_dim = tables.shape
    feats = table_feature.shape[0]
    groups = lax.axis_size("batch")
    members = lax.axis_size("mp")
    layers, width, rank = cross_down.shape
    examples = lookup_ids.shape[1] // groups
    chunks = 4
    share = examples // (chunks * members)
    tile = members * share
    mine = lookup_ids.reshape(slots_local, groups, chunks, members, share)
    mine = lax.dynamic_index_in_dim(mine, lax.axis_index("mp"), 3, keepdims=False)
    ids = jnp.transpose(mine, (1, 2, 0, 3)).reshape(-1)
    lane = jnp.arange(4 * feats, dtype=jnp.int32)
    placing = jnp.logical_and(
        (lane % 4)[:, None] == (lane // feats)[None, :],
        jnp.repeat(table_feature, 4)[:, None] == (lane % feats)[None, :],
    ).astype(BF16)
    peers = groups * members
    hbm = pl.BlockSpec(memory_space=pltpu.HBM)
    vmem = pl.BlockSpec(memory_space=pltpu.VMEM)
    dma = pltpu.SemaphoreType.DMA
    return pl.pallas_call(
        functools.partial(kernel, (groups, members, chunks, share, slot_rows)),
        out_shape=jax.ShapeDtypeStruct((examples, width), BF16),
        in_specs=[pl.BlockSpec(memory_space=pltpu.SMEM), hbm, vmem, hbm, hbm, vmem],
        out_specs=hbm,
        scratch_shapes=[
            pltpu.VMEM((slots_local * slot_rows, emb_dim), F32),
            pltpu.VMEM((share // UNROLL, UNROLL, slots_local * emb_dim), F32),
            pltpu.VMEM((256, 256), BF16),
            pltpu.VMEM((chunks, peers, 64, share), BF16),
            pltpu.VMEM((chunks, peers, 64, share), BF16),
            pltpu.VMEM((chunks, tile, width), BF16),
            pltpu.VMEM((chunks, tile, width), BF16),
            pltpu.VMEM((layers, width, rank), BF16),
            pltpu.VMEM((layers, rank, width), BF16),
            pltpu.VMEM((chunks, 2, tile // 2, rank), BF16),
            pltpu.VMEM((chunks, tile // 2, rank), BF16),
            pltpu.VMEM((chunks, tile // 2, rank), BF16),
            pltpu.VMEM((layers, chunks, tile // 2, rank), BF16),
            pltpu.VMEM((chunks, tile, rank), BF16),
            dma((chunks,)),
            dma((chunks,)),
            dma((3,)),
            dma((chunks,)),
            dma((3 * layers, chunks)),
            dma((3 * layers, chunks)),
        ],
        compiler_params=pltpu.CompilerParams(
            collective_id=0, has_side_effects=True, vmem_limit_bytes=67043328
        ),
    )(ids, tables.reshape(slots_local, peers, slot_rows // peers, share), placing, cross_down, cross_up, cross_bias)


def solution(mesh):
    return jax.shard_map(
        per_device,
        mesh=mesh,
        in_specs=(
            P("batch", None),
            P(),
            P("batch", None, None),
            P(None, "mp", None),
            P(None, None, "mp"),
            P(None, "mp"),
        ),
        out_specs=P("batch", "mp"),
        check_vma=False,
    )
```

```python
import functools

import jax
import jax.numpy as jnp
from jax import lax
from jax.experimental import pallas as pl
from jax.experimental.pallas import tpu as pltpu
from jax.sharding import PartitionSpec as P

MESH = pl.DeviceIdType.MESH
F32 = jnp.float32
BF16 = jnp.bfloat16


def kernel(
    sizes,
    ids,
    tables,
    placing,
    downs,
    ups,
    bias,
    out,
    table,
    rows_a,
    rows_b,
    pick,
    message,
    landed,
    emb,
    state,
    weight_down,
    weight_up,
    part,
    near,
    summed,
    far,
    low,
    send_sem,
    recv_sem,
    load_sem,
    out_sem,
    hop_send,
    hop_recv,
):
    groups, members, chunks, share, slot_rows = sizes
    peers = groups * members
    b = lax.axis_index("batch")
    m = lax.axis_index("mp")
    me = b * members + m
    core = lax.rem(m, 2)
    partner = {"mp": m + 1 - 2 * core}
    across = {"mp": lax.rem(m + 2, 4)}
    width = emb.shape[2]
    rank = low.shape[2]
    tile = members * share
    half = tile // 2
    mine = pl.multiple_of(core * half, half)
    theirs = pl.multiple_of((1 - core) * half, half)

    barrier = pltpu.get_barrier_semaphore()

    def greet(i, _):
        other = lax.rem(me + i, peers)
        pl.semaphore_signal(
            barrier,
            inc=1,
            device_id={"batch": other // members, "mp": lax.rem(other, members)},
            device_id_type=MESH,
        )
        return 0

    held = tables.shape[0]
    first = chunks - held
    load_table = pltpu.make_async_copy(tables, message.at[pl.ds(first, held)], load_sem.at[0])
    load_table.start()
    load_down = pltpu.make_async_copy(downs, weight_down, load_sem.at[1])
    load_down.start()
    load_up = pltpu.make_async_copy(ups, weight_up, load_sem.at[2])
    load_up.start()
    lax.fori_loop(1, peers, greet, 0)

    row = lax.broadcasted_iota(jnp.int32, (256, 256), 0)
    col = lax.broadcasted_iota(jnp.int32, (256, 256), 1)
    wanted = ((row // 4) % 2) * 128 + (row // 8) * 4 + row % 4
    pick[...] = (wanted == col).astype(BF16)

    load_table.wait()

    block_rows = message.shape[2]
    for slot in range(held):

        def widen(i, _):
            at = pl.multiple_of(slot * slot_rows + i * block_rows, block_rows)
            table[pl.ds(at, block_rows), :] = message[first + slot, i].astype(F32)
            return 0

        lax.fori_loop(0, slot_rows // block_rows, widen, 0)

    def look(rows, chunk, dest):
        first_id = (dest * chunks + chunk) * (2 * share)
        for u in range(share):
            for slot in range(2):
                index = ids[first_id + slot * share + u]
                rows[u : u + 1, slot * 128 : (slot + 1) * 128] = table[
                    pl.ds(index + slot * slot_rows, 1), :
                ]

    def packed(rows, chunk, dest):
        looked = rows[...].astype(BF16)
        message[chunk, pl.ds(dest * members, members)] = (
            lax.dot_general(
                pick[...], looked, (((1,), (1,)), ((), ())), preferred_element_type=F32
            )
            .astype(BF16)
            .reshape(members, 64, share)
        )

    def send(chunk, dest, member):
        pltpu.make_async_remote_copy(
            src_ref=message.at[chunk, dest * members + member],
            dst_ref=landed.at[chunk, me],
            send_sem=send_sem.at[chunk],
            recv_sem=recv_sem.at[chunk],
            device_id={"batch": dest, "mp": member},
            device_id_type=MESH,
        ).start()

    def to_group(chunk, dest):
        for k in range(members):
            send(chunk, dest, lax.rem(m + k, members))

    def chunk_out(chunk):
        def pair(p, _):
            left = lax.rem(b + 1 + 2 * p, groups)
            before = lax.rem(b + 2 * p, groups)
            right = lax.rem(b + 2 + 2 * p, groups)
            look(rows_a, chunk, left)
            packed(rows_b, chunk, before)

            @pl.when(p > 0)
            def _():
                to_group(chunk, before)

            look(rows_b, chunk, right)
            packed(rows_a, chunk, left)

            to_group(chunk, left)
            return 0

        lax.fori_loop(0, groups // 2, pair, 0)
        packed(rows_b, chunk, b)
        landed[chunk, me] = message[chunk, me]
        for k in range(1, members):
            send(chunk, b, lax.rem(m + k, members))

    rows_b[...] = jnp.zeros_like(rows_b)
    pl.semaphore_wait(barrier, peers - 1)

    def ahead(chunk, _):
        chunk_out(chunk)
        return 0

    lax.fori_loop(0, 2, ahead, 0)
    load_down.wait()
    load_up.wait()

    def hop(kind, t, src, dst, device):
        return pltpu.make_async_remote_copy(
            src_ref=src,
            dst_ref=dst,
            send_sem=hop_send.at[kind, t],
            recv_sem=hop_recv.at[kind, t],
            device_id=device,
            device_id_type=MESH,
        )

    def hop_near(layer, t):
        return hop(3 * layer, t, part.at[t, 1], near.at[t], partner)

    def hop_far(layer, t):
        return hop(3 * layer + 1, t, summed.at[t], far.at[layer, t], across)

    def hop_low(layer, t):
        there = low.at[t, pl.ds(mine, half)]
        return hop(3 * layer + 2, t, there, there, partner)

    def project(layer, t, source):
        for which, at in ((1, theirs), (0, mine)):
            product = jnp.dot(
                source[t, pl.ds(at, half), :], weight_down[layer], preferred_element_type=F32
            )
            part[t, which] = product.astype(BF16)
            if which == 1:
                hop_near(layer, t).start()

    def add_near(layer, t):
        hop_near(layer, t).wait()
        summed[t] = (part[t, 0].astype(F32) + near[t].astype(F32)).astype(BF16)
        hop_far(layer, t).start()

    def add_far(layer, t):
        hop_far(layer, t).wait()
        low[t, pl.ds(mine, half), :] = (
            summed[t].astype(F32) + far[layer, t].astype(F32)
        ).astype(BF16)
        hop_low(layer, t).start()

    def expand(layer, t, before):
        hop_low(layer, t).wait()

        def block(i, _):
            at = pl.ds(pl.multiple_of(i * 256, 256), 256)
            high = (
                jnp.dot(
                    low[t, at, :], weight_up[layer], preferred_element_type=F32
                )
                + bias[layer : layer + 1, :]
            )
            state[t, at, :] = (
                emb[t, at, :].astype(F32) * high + before[t, at, :].astype(F32)
            ).astype(BF16)
            return 0

        lax.fori_loop(0, tile // 256, block, 0)

    def place(t):
        pltpu.make_async_copy(
            message.at[t, pl.ds(0, peers - 1)], landed.at[t, pl.ds(0, peers - 1)], recv_sem.at[t]
        ).wait()

        def landed_of(t, i, hi):
            return jnp.concatenate(
                [landed[t, g * members + i, hi * 8 : (hi + 1) * 8, :] for g in range(groups)], axis=0
            )

        def member_rows(i, _):
            for hi in range(8):
                block = lax.dot_general(
                    landed_of(t, i, hi), placing[...], (((0,), (0,)), ((), ())), preferred_element_type=F32
                )
                emb[t, pl.ds(pl.multiple_of(i * share, share), share), hi * 256 : (hi + 1) * 256] = (
                    block.astype(BF16)
                )
            return 0

        lax.fori_loop(0, members, member_rows, 0)

    def store(t):
        return pltpu.make_async_copy(
            state.at[t], out.at[pl.ds(pl.multiple_of(t * tile, tile), tile)], out_sem.at[t]
        )

    def step(i, _):
        @pl.when(i >= 2)
        def _():
            add_far(1, i - 2)
            expand(1, i - 2, state)
            store(i - 2).start()

        @pl.when(jnp.logical_and(i >= 1, i <= chunks))
        def _():
            add_far(0, i - 1)
            expand(0, i - 1, emb)
            project(1, i - 1, state)
            add_near(1, i - 1)

        @pl.when(i < chunks)
        def _():
            place(i)
            project(0, i, emb)
            add_near(0, i)

        @pl.when(i + 2 < chunks)
        def _():
            chunk_out(i + 2)

        return 0

    lax.fori_loop(0, chunks + 2, step, 0)

    def finish(t, _):
        store(t).wait()
        pltpu.make_async_copy(
            message.at[t, pl.ds(0, peers - 1)], landed.at[t, pl.ds(0, peers - 1)], send_sem.at[t]
        ).wait()
        return 0

    lax.fori_loop(0, chunks, finish, 0)


def per_device(lookup_ids, table_feature, tables, cross_down, cross_up, cross_bias):
    slots_local, slot_rows, emb_dim = tables.shape
    feats = table_feature.shape[0]
    groups = lax.axis_size("batch")
    members = lax.axis_size("mp")
    layers, width, rank = cross_down.shape
    examples = lookup_ids.shape[1] // groups
    chunks = 4
    share = examples // (chunks * members)
    tile = members * share
    mine = lookup_ids.reshape(slots_local, groups, chunks, members, share)
    mine = lax.dynamic_index_in_dim(mine, lax.axis_index("mp"), 3, keepdims=False)
    ids = jnp.transpose(mine, (1, 2, 0, 3)).reshape(-1)
    lane = jnp.arange(4 * feats, dtype=jnp.int32)
    placing = jnp.logical_and(
        (lane % 4)[:, None] == (lane // feats)[None, :],
        jnp.repeat(table_feature, 4)[:, None] == (lane % feats)[None, :],
    ).astype(BF16)
    peers = groups * members
    hbm = pl.BlockSpec(memory_space=pltpu.HBM)
    vmem = pl.BlockSpec(memory_space=pltpu.VMEM)
    dma = pltpu.SemaphoreType.DMA
    return pl.pallas_call(
        functools.partial(kernel, (groups, members, chunks, share, slot_rows)),
        out_shape=jax.ShapeDtypeStruct((examples, width), BF16),
        in_specs=[pl.BlockSpec(memory_space=pltpu.SMEM), hbm, vmem, hbm, hbm, vmem],
        out_specs=hbm,
        scratch_shapes=[
            pltpu.VMEM((slots_local * slot_rows, emb_dim), F32),
            pltpu.VMEM((share, slots_local * emb_dim), F32),
            pltpu.VMEM((share, slots_local * emb_dim), F32),
            pltpu.VMEM((256, 256), BF16),
            pltpu.VMEM((chunks, peers, 64, share), BF16),
            pltpu.VMEM((chunks, peers, 64, share), BF16),
            pltpu.VMEM((chunks, tile, width), BF16),
            pltpu.VMEM((chunks, tile, width), BF16),
            pltpu.VMEM((layers, width, rank), BF16),
            pltpu.VMEM((layers, rank, width), BF16),
            pltpu.VMEM((chunks, 2, tile // 2, rank), BF16),
            pltpu.VMEM((chunks, tile // 2, rank), BF16),
            pltpu.VMEM((chunks, tile // 2, rank), BF16),
            pltpu.VMEM((layers, chunks, tile // 2, rank), BF16),
            pltpu.VMEM((chunks, tile, rank), BF16),
            dma((chunks,)),
            dma((chunks,)),
            dma((3,)),
            dma((chunks,)),
            dma((3 * layers, chunks)),
            dma((3 * layers, chunks)),
        ],
        compiler_params=pltpu.CompilerParams(
            collective_id=0, has_side_effects=True, vmem_limit_bytes=67043328
        ),
    )(ids, tables.reshape(slots_local, peers, slot_rows // peers, share), placing, cross_down, cross_up, cross_bias)


def solution(mesh):
    return jax.shard_map(
        per_device,
        mesh=mesh,
        in_specs=(
            P("batch", None),
            P(),
            P("batch", None, None),
            P(None, "mp", None),
            P(None, None, "mp"),
            P(None, "mp"),
        ),
        out_specs=P("batch", "mp"),
        check_vma=False,
    )
```
